32 devices in a mesh: lat: 16 (over z, y, x), dp: 2 (over core).
Axes of the slice: x: 2, y: 2, z: 4, core: 2. Of those that a mesh axis runs over, the one named last changes fastest.
Arguments:
- state: float32 [2, 128, 256, 128], P('dp', 'lat'), may hold values from -6 to 6
- cotangent: float32 [2, 128, 256, 128], P('dp', 'lat'), may hold values from -0.18 to 0.18
- w_first: bfloat16 [128, 1024], replicated, may hold values from -0.5 to 0.5
- w_middle: bfloat16 [1024, 1024], replicated, may hold values from -0.1875 to 0.1875
- w_last: bfloat16 [1024, 128], replicated, may hold values from -0.1875 to 0.1875
Outputs:
- final_state: float32 [2, 128, 256, 128], P('dp', 'lat')
- grad_first: float32 [128, 1024], replicated
- grad_middle: float32 [1024, 1024], replicated
- grad_last: float32 [1024, 128], replicated
The draws below stay inside these ranges and needn't reach their ends.
All inputs are finite; a program needn't handle non-finite values.
Results may differ from the reference program's by a relative error of at most 0.0048.
Values sent between devices are 32-bit elements; how exact they have to be, the bound alone decides.
A program may use at most 128 MiB of HBM per device.

```python
import math
import jax
import jax.numpy as jnp
from jax import lax

NLAT = 128
NLON = 256
MW = 64
FEAT = 128
HID = 1024
STEPS = 2
BATCH = 2


def shard_levels(stream_key, dims, cuts, least, top_value):
    factor_of = 1.0
    for position, blocks in cuts:
        heights = jax.random.uniform(jax.random.fold_in(jax.random.fold_in(stream_key, 6), position), (blocks,), jnp.float32, least / len(cuts), top_value / len(cuts))
        factor_of = factor_of * jnp.repeat(jnp.exp(heights), dims[position] // blocks).reshape((-1,) + (1,) * (len(dims) - 1 - position))
    return factor_of


def bell_draw(key, dims, width, most, split=(), held_as=jnp.bfloat16):
    level = shard_levels(key, dims, split, -0.22, 0.18) if split else 1.0
    values = jax.random.normal(key, dims, jnp.float32) * width * level
    return jnp.minimum(jnp.maximum(values, -most), most).astype(held_as)


def setup_inputs(seed: int = 0) -> dict:
    seeds = jax.random.split(jax.random.key(seed), 6)
    return {
        "state": bell_draw(seeds[0], (BATCH, NLAT, NLON, FEAT), 1.0, 6.0, ((0, 2), (1, 16)), jnp.float32),
        "cotangent": bell_draw(seeds[1], (BATCH, NLAT, NLON, FEAT), 0.03, 0.18, ((0, 2), (1, 16)), jnp.float32),
        "w_first": bell_draw(seeds[2], (FEAT, HID), FEAT ** -0.5, 0.5),
        "w_middle": bell_draw(seeds[3], (HID, HID), HID ** -0.5, 0.1875),
        "w_last": bell_draw(seeds[4], (HID, FEAT), HID ** -0.5, 0.1875),
    }


highest = lax.Precision.HIGHEST
tend_weight = 0.5

def grid_tables(lon_count, wave_count):
    lon_index = jnp.arange(lon_count, dtype=jnp.int32)
    wave_index = jnp.arange(wave_count, dtype=jnp.int32)
    phase_angle = (lon_index[:, None] * wave_index[None, :] % lon_count).astype(jnp.float32) * (2.0 * math.pi / lon_count)
    cosine = jnp.cos(phase_angle)
    sine_part = jnp.sin(phase_angle)
    analysis = jnp.stack([cosine, -sine_part], axis=2) / lon_count
    factor = jnp.where(wave_index == 0, 1.0, 2.0).astype(jnp.float32)
    synthesis = jnp.stack([cosine, -sine_part], axis=2) * factor[None, :, None]
    return (analysis, synthesis)

def legendre(wave_ids, lat_count, wave_count):
    lat_index = jnp.arange(lat_count).astype(jnp.float32)
    latitude = (lat_index + 0.5) * (math.pi / lat_count) - 0.5 * math.pi
    sine_lat = jnp.sin(latitude)
    cosine_lat = jnp.cos(latitude)
    quad_weight = cosine_lat * (math.pi / lat_count)
    order_m = wave_ids.astype(jnp.float32)
    counter = jnp.arange(1, wave_count).astype(jnp.float32)
    increments = 0.5 * jnp.log((2.0 * counter + 1.0) / (2.0 * counter))
    summed = lax.optimization_barrier(jnp.sum(jnp.where(counter[None, :] <= order_m[:, None], increments[None, :], 0.0), axis=1))
    diagonal = jnp.exp(0.5 * math.log(0.5) + summed[:, None] + order_m[:, None] * jnp.log(cosine_lat)[None, :])

    def advance(carry, offset):
        previous, current, ratio_prev = carry
        degree = order_m + offset
        ratio_new = jnp.sqrt((4.0 * degree * degree - 1.0) / (degree * degree - order_m * order_m))
        following = ratio_new[:, None] * (sine_lat[None, :] * current - previous / ratio_prev[:, None])
        return ((current, following, ratio_new), following)
    initial = (jnp.zeros_like(diagonal), diagonal, jnp.ones_like(order_m))
    _, remaining = lax.scan(advance, initial, jnp.arange(1, wave_count).astype(jnp.float32))
    poly_table = jnp.concatenate([diagonal[None], remaining], axis=0).transpose(1, 0, 2)
    degree = order_m[:, None] + jnp.arange(wave_count).astype(jnp.float32)[None, :]
    kept_mask = degree <= wave_count - 1
    poly_table = jnp.where(kept_mask[:, :, None], poly_table, 0.0)
    damping = jnp.where(kept_mask, 1.0 / (1.0 + degree * (degree + 1.0) / (wave_count * (wave_count - 1.0))), 0.0)
    return (poly_table, quad_weight, damping)

def spectral_whole(field, first, last, in_table, out_table, damping):
    wave_grid = jnp.einsum('bjxf,xmp->bjmpf', field, first, precision=highest)
    coeffs = jnp.einsum('mkj,bjmpf->bmkpf', in_table, wave_grid, precision=highest) * damping[None, :, :, None, None]
    back_grid = jnp.einsum('mkj,bmkpf->bjmpf', out_table, coeffs, precision=highest)
    return jnp.einsum('bjmpf,xmp->bjxf', back_grid, last, precision=highest)

def silu_slope(value):
    gate_sig = jax.nn.sigmoid(value)
    return gate_sig * (1.0 + value * (1.0 - gate_sig))

def hidden_rows(rows, w_first, w_middle):
    pre_first = jnp.dot(rows, w_first, preferred_element_type=jnp.float32)
    hidden_first = jax.nn.silu(pre_first).astype(jnp.bfloat16)
    pre_middle = jnp.dot(hidden_first, w_middle, preferred_element_type=jnp.float32)
    hidden_middle = jax.nn.silu(pre_middle).astype(jnp.bfloat16)
    return (pre_first, hidden_first, pre_middle, hidden_middle)

def forward_rows(rows, w_first, w_middle, w_last):
    _, _, _, hidden_middle = hidden_rows(rows, w_first, w_middle)
    return jnp.dot(hidden_middle, w_last, preferred_element_type=jnp.float32)

def backward_rows(rows, scaled, w_first, w_middle, w_last):
    pre_first, hidden_first, pre_middle, hidden_middle = hidden_rows(rows, w_first, w_middle)
    grad_last = jnp.dot(hidden_middle.T, scaled, preferred_element_type=jnp.float32)
    middle_back = jnp.dot(scaled, w_last.T, preferred_element_type=jnp.float32)
    middle_grad = (middle_back * silu_slope(pre_middle)).astype(jnp.bfloat16)
    grad_middle = jnp.dot(hidden_first.T, middle_grad, preferred_element_type=jnp.float32)
    first_back = jnp.dot(middle_grad, w_middle.T, preferred_element_type=jnp.float32)
    first_grad = (first_back * silu_slope(pre_first)).astype(jnp.bfloat16)
    grad_first = jnp.dot(rows.T, first_grad, preferred_element_type=jnp.float32)
    back_rows = jnp.dot(first_grad, w_first.T, preferred_element_type=jnp.float32)
    return ((grad_first, grad_middle, grad_last), back_rows)

def reference(state, cotangent, w_first, w_middle, w_last):
    batch, lat_count, lon_count, features = state.shape
    hidden_count = w_first.shape[1]
    analysis, synthesis = grid_tables(lon_count, MW)
    poly_table, quad_weight, damping = legendre(jnp.arange(MW, dtype=jnp.int32), lat_count, MW)
    weighted = poly_table * quad_weight[None, None, :]
    row_count = batch * lat_count * lon_count
    block = math.gcd(row_count, 8192)
    inputs = []
    field = state
    for step_index in range(STEPS):
        inputs.append(field)
        rows = field.reshape(row_count // block, block, features).astype(jnp.bfloat16)
        tendency = lax.map(lambda piece: forward_rows(piece, w_first, w_middle, w_last), rows)
        moved = field + tend_weight * tendency.reshape(field.shape)
        field = spectral_whole(moved, analysis, synthesis, weighted, poly_table, damping)
    final_state = field
    grad = cotangent
    totals = (jnp.zeros((features, hidden_count), jnp.float32), jnp.zeros((hidden_count, hidden_count), jnp.float32), jnp.zeros((hidden_count, features), jnp.float32))
    for step_index in reversed(range(STEPS)):
        pulled = spectral_whole(grad, synthesis, analysis, poly_table, weighted, damping)
        scaled = (tend_weight * pulled).astype(jnp.bfloat16).reshape(row_count // block, block, features)
        rows = inputs[step_index].reshape(row_count // block, block, features).astype(jnp.bfloat16)

        def accumulate(carry, pieces):
            grads, back_rows = backward_rows(pieces[0], pieces[1], w_first, w_middle, w_last)
            return ((carry[0] + grads[0], carry[1] + grads[1], carry[2] + grads[2]), back_rows)
        totals, back_rows = lax.scan(accumulate, totals, (rows, scaled))
        grad = pulled + back_rows.reshape(field.shape)
    return (final_state, totals[0], totals[1], totals[2])
```

```python
import functools
import math

import jax
import jax.numpy as jnp
import numpy as np
from jax import lax
from jax.experimental import pallas as pl
from jax.experimental.pallas import tpu as pltpu
from jax.sharding import PartitionSpec as P

MW = 64
STEPS = 2

high = lax.Precision.HIGH
tend_weight = 0.5


def grid_tables(lon_count, wave_count):
    lon_index = np.arange(lon_count)
    wave_index = np.arange(wave_count)
    angle = 2.0 * math.pi * (lon_index[:, None] * wave_index[None, :] % lon_count) / lon_count
    pair = np.stack([np.cos(angle), -np.sin(angle)], axis=2)
    factor = np.where(wave_index == 0, 1.0, 2.0)
    analysis = (pair / lon_count).reshape(lon_count, -1).astype(np.float32)
    synthesis = (pair * factor[None, :, None]).reshape(lon_count, -1).astype(np.float32)
    return analysis, synthesis


def legendre_tables(lat_count, wave_count):
    latitude = -0.5 * math.pi + (np.arange(lat_count) + 0.5) * math.pi / lat_count
    mu, cosine = np.sin(latitude), np.cos(latitude)
    quad_weight = cosine * math.pi / lat_count
    order = np.arange(wave_count, dtype=np.float64)
    steps = np.concatenate([[0.0], 0.5 * np.log((2 * order[1:] + 1) / (2 * order[1:]))])
    diagonal = np.exp(
        0.5 * math.log(0.5) + np.cumsum(steps)[:, None] + order[:, None] * np.log(cosine)[None, :]
    )
    rows = [diagonal]
    previous, current, ratio_prev = np.zeros_like(diagonal), diagonal, np.ones_like(order)
    for offset in range(1, wave_count):
        n = order + offset
        ratio = np.sqrt((4 * n * n - 1) / (n * n - order * order))
        following = ratio[:, None] * (mu[None, :] * current - previous / ratio_prev[:, None])
        previous, current, ratio_prev = current, following, ratio
        rows.append(following)
    table = np.stack(rows, axis=1)
    degree = order[:, None] + np.arange(wave_count)[None, :]
    kept = degree <= wave_count - 1
    damping = np.where(kept, 1.0 / (1.0 + degree * (degree + 1) / (wave_count * (wave_count - 1.0))), 0.0)
    table = np.where(kept[:, :, None], table, 0.0) * np.sqrt(damping)[:, :, None]
    return table.astype(np.float32), quad_weight.astype(np.float32)


def silu_pair(value):
    gate = 0.5 * jnp.tanh(0.5 * value) + 0.5
    hidden = value * gate
    return hidden, gate + hidden - hidden * gate


def forward_kernel(x_ref, w1_ref, w2_ref, w3_ref, moved_ref, h1_ref, s1_ref, h2_ref, s2_ref):
    field = x_ref[...]
    rows = field.astype(jnp.bfloat16)
    h1, s1 = silu_pair(jnp.dot(rows, w1_ref[...], preferred_element_type=jnp.float32))
    h1 = h1.astype(jnp.bfloat16)
    h1_ref[...] = h1
    s1_ref[...] = s1.astype(jnp.bfloat16)
    h2, s2 = silu_pair(jnp.dot(h1, w2_ref[...], preferred_element_type=jnp.float32))
    h2 = h2.astype(jnp.bfloat16)
    h2_ref[...] = h2
    s2_ref[...] = s2.astype(jnp.bfloat16)
    tend = jnp.dot(h2, w3_ref[...], preferred_element_type=jnp.float32)
    moved_ref[...] = field + tend_weight * tend


def forward_rows(x, w1, w2, w3):
    count, features = x.shape
    hidden = w1.shape[1]
    tile = math.gcd(count, 256)
    row = lambda width: pl.BlockSpec((tile, width), lambda i: (i, 0))
    whole = lambda w: pl.BlockSpec(w.shape, lambda i: (0, 0))
    wide = jax.ShapeDtypeStruct((count, hidden), jnp.bfloat16)
    return pl.pallas_call(
        forward_kernel,
        grid=(count // tile,),
        in_specs=[row(features), whole(w1), whole(w2), whole(w3)],
        out_specs=[row(features)] + [row(hidden)] * 4,
        out_shape=[jax.ShapeDtypeStruct(x.shape, jnp.float32)] + [wide] * 4,
        cost_estimate=pl.CostEstimate(
            flops=2 * count * (2 * features * hidden + hidden * hidden),
            bytes_accessed=count * hidden * 8, transcendentals=2 * count * hidden,
        ),
        compiler_params=pltpu.CompilerParams(dimension_semantics=("arbitrary",)),
    )(x, w1, w2, w3)


def mul_t(a, b):
    return lax.dot_general(a, b, (((1,), (1,)), ((), ())), preferred_element_type=jnp.float32)


def t_mul(a, b):
    return lax.dot_general(a, b, (((0,), (0,)), ((), ())), preferred_element_type=jnp.float32)


def backward_kernel(first_call, need_rows, *refs):
    p_ref, x_ref, h1_ref, s1_ref, h2_ref, s2_ref, w1_ref, w2_ref, w3_ref = refs[:9]
    refs = refs[9:]
    if not first_call:
        c1_ref, c2_ref, c3_ref = refs[:3]
        refs = refs[3:]
    g1_ref, g2_ref, g3_ref = refs[:3]

    @pl.when(pl.program_id(0) == 0)
    def _():
        if first_call:
            g1_ref[...] = jnp.zeros_like(g1_ref)
            g2_ref[...] = jnp.zeros_like(g2_ref)
            g3_ref[...] = jnp.zeros_like(g3_ref)
        else:
            g1_ref[...] = c1_ref[...]
            g2_ref[...] = c2_ref[...]
            g3_ref[...] = c3_ref[...]

    pulled = p_ref[...]
    gt = (tend_weight * pulled).astype(jnp.bfloat16)
    g3_ref[...] += t_mul(h2_ref[...], gt)
    ga2 = (mul_t(gt, w3_ref[...]) * s2_ref[...].astype(jnp.float32)).astype(jnp.bfloat16)
    g2_ref[...] += t_mul(h1_ref[...], ga2)
    ga1 = (mul_t(ga2, w2_ref[...]) * s1_ref[...].astype(jnp.float32)).astype(jnp.bfloat16)
    g1_ref[...] += t_mul(x_ref[...].astype(jnp.bfloat16), ga1)
    if need_rows:
        refs[3][...] = pulled + mul_t(ga1, w1_ref[...])


def backward_rows(pulled, x, saved, w1, w2, w3, carry, need_rows):
    count, features = x.shape
    hidden = w1.shape[1]
    tile = math.gcd(count, 512)
    row = lambda width: pl.BlockSpec((tile, width), lambda i: (i, 0))
    whole = lambda w: pl.BlockSpec(w.shape, lambda i: (0, 0))
    out_shape = [jax.ShapeDtypeStruct(w.shape, jnp.float32) for w in (w1, w2, w3)]
    out_specs = [whole(w) for w in (w1, w2, w3)]
    carried = [] if carry is None else list(carry)
    if need_rows:
        out_shape.append(jax.ShapeDtypeStruct(x.shape, jnp.float32))
        out_specs.append(row(features))
    return pl.pallas_call(
        functools.partial(backward_kernel, carry is None, need_rows),
        grid=(count // tile,),
        in_specs=[row(features)] * 2 + [row(hidden)] * 4
        + [whole(w) for w in (w1, w2, w3)] + [whole(c) for c in carried],
        out_specs=out_specs,
        out_shape=out_shape,
        cost_estimate=pl.CostEstimate(
            flops=4 * count * (2 * features * hidden + hidden * hidden),
            bytes_accessed=count * hidden * 8, transcendentals=0,
        ),
        compiler_params=pltpu.CompilerParams(dimension_semantics=("arbitrary",)),
    )(pulled, x, *saved, w1, w2, w3, *carried)


def body(state, cotangent, w1, w2, w3):
    sample, lat_rows, lon_count, features = state.shape
    bands = lax.axis_size("lat")
    lat_count = lat_rows * bands
    waves = MW // bands
    analysis, synthesis = grid_tables(lon_count, MW)
    table, quad = legendre_tables(lat_count, MW)
    mine = lax.dynamic_slice_in_dim(jnp.asarray(table), lax.axis_index("lat") * waves, waves, axis=0)
    base = jnp.einsum("mki,mkj->mij", mine, mine, precision=lax.Precision.HIGHEST)
    quad = jnp.asarray(quad)
    forward_op = base * quad[None, None, :]
    backward_op = base * quad[None, :, None]

    def spectral(parts):
        sent = []
        for field, first, _, _ in parts:
            wav = jnp.einsum("bjxf,xq->bqjf", field, first, precision=high)
            sent.append(wav.reshape(sample, bands, waves * 2, lat_rows, features))
        sent = jnp.concatenate(sent, axis=0).transpose(1, 0, 2, 3, 4)
        got = lax.all_to_all(sent, "lat", split_axis=0, concat_axis=0, tiled=True)
        got = got.reshape(bands, len(parts), sample, waves, 2, lat_rows, features)
        ops = jnp.stack([p[2] for p in parts]).reshape(len(parts), waves, bands, lat_rows, lat_count)
        got = got.transpose(1, 3, 0, 5, 2, 4, 6).reshape(len(parts), waves, lat_count, -1)
        ops = ops.reshape(len(parts), waves, lat_count, lat_count)
        back = jnp.einsum("smij,smjv->smiv", ops, got, precision=high)
        back = back.reshape(len(parts), waves, bands, lat_rows, sample, 2, features)
        back = back.transpose(2, 0, 4, 1, 5, 3, 6)
        back = lax.all_to_all(back, "lat", split_axis=0, concat_axis=0, tiled=True)
        out = []
        for index, (_, _, _, last) in enumerate(parts):
            piece = back[:, index].transpose(1, 0, 2, 3, 4, 5)
            piece = piece.reshape(sample, MW * 2, lat_rows, features)
            out.append(jnp.einsum("bqjf,xq->bjxf", piece, last, precision=high))
        return out

    flat = lambda field: field.reshape(sample * lat_rows * lon_count, features)
    x0 = flat(state)
    moved0, *saved0 = forward_rows(x0, w1, w2, w3)
    q1, pulled1 = spectral([
        (moved0.reshape(state.shape), analysis, forward_op, synthesis),
        (cotangent, synthesis, backward_op, analysis),
    ])
    x1 = flat(q1)
    moved1, *saved1 = forward_rows(x1, w1, w2, w3)
    *totals, grad = backward_rows(flat(pulled1), x1, saved1, w1, w2, w3, None, True)
    final, pulled0 = spectral([
        (moved1.reshape(state.shape), analysis, forward_op, synthesis),
        (grad.reshape(state.shape), synthesis, backward_op, analysis),
    ])
    totals = backward_rows(flat(pulled0), x0, saved0, w1, w2, w3, totals, False)
    totals = reduce_totals(totals)
    return (final, *totals)


def reduce_totals(totals):
    return lax.psum(tuple(totals), ("lat", "dp"))


def solution(mesh):
    field = P("dp", "lat", None, None)
    return jax.shard_map(
        body, mesh=mesh, in_specs=(field, field, P(), P(), P()),
        out_specs=(field, P(), P(), P()), check_vma=False,
    )
```

```python
import functools
import math

import jax
import jax.numpy as jnp
import numpy as np
from jax import lax
from jax.experimental import pallas as pl
from jax.experimental.pallas import tpu as pltpu
from jax.sharding import PartitionSpec as P

MW = 64
STEPS = 2

high = lax.Precision.HIGH
tend_weight = 0.5


def grid_tables(lon_count, wave_count):
    lon_index = np.arange(lon_count)
    wave_index = np.arange(wave_count)
    angle = 2.0 * math.pi * (lon_index[:, None] * wave_index[None, :] % lon_count) / lon_count
    pair = np.stack([np.cos(angle), -np.sin(angle)], axis=2)
    factor = np.where(wave_index == 0, 1.0, 2.0)
    analysis = (pair / lon_count).reshape(lon_count, -1).astype(np.float32)
    synthesis = (pair * factor[None, :, None]).reshape(lon_count, -1).astype(np.float32)
    return analysis, synthesis


def legendre_tables(lat_count, wave_count):
    latitude = -0.5 * math.pi + (np.arange(lat_count) + 0.5) * math.pi / lat_count
    mu, cosine = np.sin(latitude), np.cos(latitude)
    quad_weight = cosine * math.pi / lat_count
    order = np.arange(wave_count, dtype=np.float64)
    steps = np.concatenate([[0.0], 0.5 * np.log((2 * order[1:] + 1) / (2 * order[1:]))])
    diagonal = np.exp(
        0.5 * math.log(0.5) + np.cumsum(steps)[:, None] + order[:, None] * np.log(cosine)[None, :]
    )
    rows = [diagonal]
    previous, current, ratio_prev = np.zeros_like(diagonal), diagonal, np.ones_like(order)
    for offset in range(1, wave_count):
        n = order + offset
        ratio = np.sqrt((4 * n * n - 1) / (n * n - order * order))
        following = ratio[:, None] * (mu[None, :] * current - previous / ratio_prev[:, None])
        previous, current, ratio_prev = current, following, ratio
        rows.append(following)
    table = np.stack(rows, axis=1)
    degree = order[:, None] + np.arange(wave_count)[None, :]
    kept = degree <= wave_count - 1
    damping = np.where(kept, 1.0 / (1.0 + degree * (degree + 1) / (wave_count * (wave_count - 1.0))), 0.0)
    table = np.where(kept[:, :, None], table, 0.0) * np.sqrt(damping)[:, :, None]
    return table.astype(np.float32), quad_weight.astype(np.float32)


def silu_pair(value):
    gate = 0.5 * jnp.tanh(0.5 * value) + 0.5
    hidden = value * gate
    return hidden, gate + hidden - hidden * gate


def forward_kernel(x_ref, w1_ref, w2_ref, w3_ref, moved_ref, h1_ref, s1_ref, h2_ref, s2_ref):
    field = x_ref[...]
    rows = field.astype(jnp.bfloat16)
    h1, s1 = silu_pair(jnp.dot(rows, w1_ref[...], preferred_element_type=jnp.float32))
    h1 = h1.astype(jnp.bfloat16)
    h1_ref[...] = h1
    s1_ref[...] = s1.astype(jnp.bfloat16)
    h2, s2 = silu_pair(jnp.dot(h1, w2_ref[...], preferred_element_type=jnp.float32))
    h2 = h2.astype(jnp.bfloat16)
    h2_ref[...] = h2
    s2_ref[...] = s2.astype(jnp.bfloat16)
    tend = jnp.dot(h2, w3_ref[...], preferred_element_type=jnp.float32)
    moved_ref[...] = field + tend_weight * tend


def forward_rows(x, w1, w2, w3):
    count, features = x.shape
    hidden = w1.shape[1]
    tile = math.gcd(count, 256)
    row = lambda width: pl.BlockSpec((tile, width), lambda i: (i, 0))
    whole = lambda w: pl.BlockSpec(w.shape, lambda i: (0, 0))
    wide = jax.ShapeDtypeStruct((count, hidden), jnp.bfloat16)
    return pl.pallas_call(
        forward_kernel,
        grid=(count // tile,),
        in_specs=[row(features), whole(w1), whole(w2), whole(w3)],
        out_specs=[row(features)] + [row(hidden)] * 4,
        out_shape=[jax.ShapeDtypeStruct(x.shape, jnp.float32)] + [wide] * 4,
        cost_estimate=pl.CostEstimate(
            flops=2 * count * (2 * features * hidden + hidden * hidden),
            bytes_accessed=count * hidden * 8, transcendentals=2 * count * hidden,
        ),
        compiler_params=pltpu.CompilerParams(dimension_semantics=("arbitrary",)),
    )(x, w1, w2, w3)


def mul_t(a, b):
    return lax.dot_general(a, b, (((1,), (1,)), ((), ())), preferred_element_type=jnp.float32)


def t_mul(a, b):
    return lax.dot_general(a, b, (((0,), (0,)), ((), ())), preferred_element_type=jnp.float32)


def backward_kernel(first_call, need_rows, *refs):
    p_ref, x_ref, h1_ref, s1_ref, h2_ref, s2_ref, w1_ref, w2_ref, w3_ref = refs[:9]
    refs = refs[9:]
    if not first_call:
        c1_ref, c2_ref, c3_ref = refs[:3]
        refs = refs[3:]
    g1_ref, g2_ref, g3_ref = refs[:3]

    @pl.when(pl.program_id(0) == 0)
    def _():
        if first_call:
            g1_ref[...] = jnp.zeros_like(g1_ref)
            g2_ref[...] = jnp.zeros_like(g2_ref)
            g3_ref[...] = jnp.zeros_like(g3_ref)
        else:
            g1_ref[...] = c1_ref[...]
            g2_ref[...] = c2_ref[...]
            g3_ref[...] = c3_ref[...]

    pulled = p_ref[...]
    gt = (tend_weight * pulled).astype(jnp.bfloat16)
    g3_ref[...] += t_mul(h2_ref[...], gt)
    ga2 = (mul_t(gt, w3_ref[...]) * s2_ref[...].astype(jnp.float32)).astype(jnp.bfloat16)
    g2_ref[...] += t_mul(h1_ref[...], ga2)
    ga1 = (mul_t(ga2, w2_ref[...]) * s1_ref[...].astype(jnp.float32)).astype(jnp.bfloat16)
    g1_ref[...] += t_mul(x_ref[...].astype(jnp.bfloat16), ga1)
    if need_rows:
        refs[3][...] = pulled + mul_t(ga1, w1_ref[...])


def backward_rows(pulled, x, saved, w1, w2, w3, carry, need_rows):
    count, features = x.shape
    hidden = w1.shape[1]
    tile = math.gcd(count, 512)
    row = lambda width: pl.BlockSpec((tile, width), lambda i: (i, 0))
    whole = lambda w: pl.BlockSpec(w.shape, lambda i: (0, 0))
    out_shape = [jax.ShapeDtypeStruct(w.shape, jnp.float32) for w in (w1, w2, w3)]
    out_specs = [whole(w) for w in (w1, w2, w3)]
    carried = [] if carry is None else list(carry)
    if need_rows:
        out_shape.append(jax.ShapeDtypeStruct(x.shape, jnp.float32))
        out_specs.append(row(features))
    return pl.pallas_call(
        functools.partial(backward_kernel, carry is None, need_rows),
        grid=(count // tile,),
        in_specs=[row(features)] * 2 + [row(hidden)] * 4
        + [whole(w) for w in (w1, w2, w3)] + [whole(c) for c in carried],
        out_specs=out_specs,
        out_shape=out_shape,
        cost_estimate=pl.CostEstimate(
            flops=4 * count * (2 * features * hidden + hidden * hidden),
            bytes_accessed=count * hidden * 8, transcendentals=0,
        ),
        compiler_params=pltpu.CompilerParams(dimension_semantics=("arbitrary",)),
    )(pulled, x, *saved, w1, w2, w3, *carried)


def body(state, cotangent, w1, w2, w3):
    sample, lat_rows, lon_count, features = state.shape
    bands = lax.axis_size("lat")
    lat_count = lat_rows * bands
    waves = MW // bands
    analysis, synthesis = grid_tables(lon_count, MW)
    table, quad = legendre_tables(lat_count, MW)
    mine = lax.dynamic_slice_in_dim(jnp.asarray(table), lax.axis_index("lat") * waves, waves, axis=0)
    base = jnp.einsum("mki,mkj->mij", mine, mine, precision=lax.Precision.HIGHEST)
    quad = jnp.asarray(quad)
    forward_op = base * quad[None, None, :]
    backward_op = base * quad[None, :, None]

    def spectral(parts):
        sent = []
        for field, first, _, _ in parts:
            wav = jnp.einsum("bjxf,xq->bqjf", field, first, precision=high)
            sent.append(wav.reshape(sample, bands, waves * 2, lat_rows, features))
        sent = jnp.concatenate(sent, axis=0).transpose(1, 0, 2, 3, 4)
        got = lax.all_to_all(sent, "lat", split_axis=0, concat_axis=0, tiled=True)
        got = got.reshape(bands, len(parts), sample, waves, 2, lat_rows, features)
        ops = jnp.stack([p[2] for p in parts]).reshape(len(parts), waves, bands, lat_rows, lat_count)
        got = got.transpose(1, 3, 0, 5, 2, 4, 6).reshape(len(parts), waves, lat_count, -1)
        ops = ops.reshape(len(parts), waves, lat_count, lat_count)
        back = jnp.einsum("smij,smjv->smiv", ops, got, precision=high)
        back = back.reshape(len(parts), waves, bands, lat_rows, sample, 2, features)
        back = back.transpose(2, 0, 4, 1, 5, 3, 6)
        back = lax.all_to_all(back, "lat", split_axis=0, concat_axis=0, tiled=True)
        out = []
        for index, (_, _, _, last) in enumerate(parts):
            piece = back[:, index].transpose(1, 0, 2, 3, 4, 5)
            piece = piece.reshape(sample, MW * 2, lat_rows, features)
            out.append(jnp.einsum("bqjf,xq->bjxf", piece, last, precision=high))
        return out

    flat = lambda field: field.reshape(sample * lat_rows * lon_count, features)
    x0 = flat(state)
    moved0, *saved0 = forward_rows(x0, w1, w2, w3)
    (pulled1,) = spectral([(cotangent, synthesis, backward_op, analysis)])
    (q1,) = spectral([(moved0.reshape(state.shape), analysis, forward_op, synthesis)])
    x1 = flat(q1)
    moved1, *saved1 = forward_rows(x1, w1, w2, w3)
    *totals, grad = backward_rows(flat(pulled1), x1, saved1, w1, w2, w3, None, True)
    (final,) = spectral([(moved1.reshape(state.shape), analysis, forward_op, synthesis)])
    (pulled0,) = spectral([(grad.reshape(state.shape), synthesis, backward_op, analysis)])
    totals = backward_rows(flat(pulled0), x0, saved0, w1, w2, w3, totals, False)
    totals = reduce_totals(totals)
    return (final, *totals)


def reduce_totals(totals):
    return lax.psum(tuple(totals), ("lat", "dp"))


def solution(mesh):
    field = P("dp", "lat", None, None)
    return jax.shard_map(
        body, mesh=mesh, in_specs=(field, field, P(), P(), P()),
        out_specs=(field, P(), P(), P()), check_vma=False,
    )
```
